32 devices in a mesh: row: 4 (over x, core), col: 8 (over z, y).
Axes of the slice: x: 2, y: 2, z: 4, core: 2. Of those that a mesh axis runs over, the one named last changes fastest.
Arguments:
- rhs_c: float32 [12, 512, 6, 1024], P(None, 'row', None, 'col'), may hold values from -6 to 6
- rhs_f: float32 [12, 512, 6, 1024], P(None, 'row', None, 'col'), may hold values from -6 to 6
- pencil_a: bfloat16 [12, 512, 6, 1024], P(None, 'row', None, 'col'), may hold values from -0.5 to 0.5
- pencil_d: bfloat16 [12, 512, 6, 1024], P(None, 'row', None, 'col'), may hold values from -0.5 to 0.5
- pencil_b: bfloat16 [12, 512, 6, 1024], P(None, 'row', None, 'col'), may hold values from -0.5 to 0.5
- pencil_e: bfloat16 [12, 512, 6, 1024], P(None, 'row', None, 'col'), may hold values from -0.5 to 0.5
- d_inverse: float32 [12, 512, 128], P(None, 'row'), may hold values from -0.25 to 2.5
- left_vectors: float32 [12, 512, 128], P(None, 'row'), may hold values from -0.25 to 2.5
- left_inverse: float32 [12, 512, 128], P(None, 'row'), may hold values from -0.25 to 2.5
- left_eigs: float32 [12, 512], P(None, 'row'), may hold values from 1 to 3
- e_inverse: float32 [6, 1024, 128], P(None, 'col'), may hold values from -0.25 to 2.5
- right_vectors: float32 [6, 1024, 128], P(None, 'col'), may hold values from -0.25 to 2.5
- right_inverse: float32 [6, 1024, 128], P(None, 'col'), may hold values from -0.25 to 2.5
- right_eigs: float32 [6, 1024], P(None, 'col'), may hold values from -3 to -1
Outputs:
- updated_c: float32 [12, 512, 6, 1024], P(None, 'row', None, 'col')
- updated_f: float32 [12, 512, 6, 1024], P(None, 'row', None, 'col')
- solved_r: float32 [12, 512, 6, 1024], P(None, 'row', None, 'col')
- solved_l: float32 [12, 512, 6, 1024], P(None, 'row', None, 'col')
The draws below stay inside these ranges and needn't reach their ends.
All inputs are finite; a program needn't handle non-finite values.
Results may differ from the reference program's by a relative error of at most 0.0003.
Values may be sent and summed in bfloat16 or wider, within the bound.
A program may use at most 128 MiB of HBM per device.

```python
import math
import jax
import jax.numpy as jnp
from jax import lax

TILE = 128
ORDER = 6144
STEPS = 3
RT = 12
CT = 6
N_ROW = 4
N_COL = 8


def dominant(key, lead, height, salt):
    key = jax.random.fold_in(key, salt)
    first, second = jax.random.split(key)
    shape = (lead, height, TILE)
    diagonal = jnp.exp(jax.random.uniform(first, shape, jnp.float32, 0.0, math.log(2.0)))
    spread = jnp.clip(0.4 / math.sqrt(TILE) * jax.random.normal(second, shape, jnp.float32), -0.25, 0.25)
    rows = lax.broadcasted_iota(jnp.int32, shape, 1) % TILE
    cols = lax.broadcasted_iota(jnp.int32, shape, 2)
    return jnp.where(rows == cols, diagonal, spread)


def draw_d_inverse(key, part):
    return dominant(key, RT, N_ROW * TILE, 11)


def draw_left_vectors(key, part):
    return dominant(key, RT, N_ROW * TILE, 12)


def draw_left_inverse(key, part):
    return dominant(key, RT, N_ROW * TILE, 13)


def draw_e_inverse(key, part):
    return dominant(key, CT, N_COL * TILE, 14)


def draw_right_vectors(key, part):
    return dominant(key, CT, N_COL * TILE, 15)


def draw_right_inverse(key, part):
    return dominant(key, CT, N_COL * TILE, 16)


def levels(stream_key, dims, shards, low, top_value):
    def one(dim, blocks):
        steps = jax.random.uniform(jax.random.fold_in(jax.random.fold_in(stream_key, 6), dim), (blocks,), jnp.float32, low / len(shards), top_value / len(shards))
        return jnp.repeat(jnp.exp(steps), dims[dim] // blocks).reshape((-1,) + (1,) * (len(dims) - dim - 1))

    factor_of = one(*shards[0])
    for cut in shards[1:]:
        factor_of = factor_of * one(*cut)
    return factor_of


def scatter_about(key, extent, width, limit, cuts=(), kind=jnp.bfloat16):
    entries = width * jax.random.normal(key, extent, jnp.float32)
    if cuts:
        entries = entries * levels(key, extent, cuts, -0.22, 0.18)
    return jnp.clip(entries, -limit, limit).astype(kind)


def setup_inputs(seed: int = 0) -> dict:
    seeds = jax.random.split(jax.random.key(seed), 15)
    return {
        "rhs_c": scatter_about(seeds[0], (RT, N_ROW * TILE, CT, N_COL * TILE), 1.0, 6.0, ((1, 4), (3, 8)), jnp.float32),
        "rhs_f": scatter_about(seeds[1], (RT, N_ROW * TILE, CT, N_COL * TILE), 1.0, 6.0, ((1, 4), (3, 8)), jnp.float32),
        "pencil_a": scatter_about(seeds[2], (RT, N_ROW * TILE, CT, N_COL * TILE), TILE ** -0.5, 0.5, ((1, 4), (3, 8))),
        "pencil_d": scatter_about(seeds[3], (RT, N_ROW * TILE, CT, N_COL * TILE), TILE ** -0.5, 0.5, ((1, 4), (3, 8))),
        "pencil_b": scatter_about(seeds[4], (RT, N_ROW * TILE, CT, N_COL * TILE), TILE ** -0.5, 0.5, ((1, 4), (3, 8))),
        "pencil_e": scatter_about(seeds[5], (RT, N_ROW * TILE, CT, N_COL * TILE), TILE ** -0.5, 0.5, ((1, 4), (3, 8))),
        "d_inverse": draw_d_inverse(jax.random.fold_in(seeds[14], 71), 0),
        "left_vectors": draw_left_vectors(jax.random.fold_in(seeds[14], 71), 0),
        "left_inverse": draw_left_inverse(jax.random.fold_in(seeds[14], 71), 0),
        "left_eigs": jnp.clip(jnp.exp(math.log(3.0) - 1.0986123 * jax.random.uniform(seeds[9], (RT, N_ROW * TILE), jnp.float32) ** levels(seeds[9], (RT, N_ROW * TILE), ((1, 4),), -0.2, 0.2)), 1.0, 3.0),
        "e_inverse": draw_e_inverse(jax.random.fold_in(seeds[14], 71), 0),
        "right_vectors": draw_right_vectors(jax.random.fold_in(seeds[14], 71), 0),
        "right_inverse": draw_right_inverse(jax.random.fold_in(seeds[14], 71), 0),
        "right_eigs": jnp.clip(-3.0 + 2.0 * jax.random.uniform(seeds[13], (CT, N_COL * TILE), jnp.float32) ** levels(seeds[13], (CT, N_COL * TILE), ((1, 8),), -0.2, 0.2), -3.0, -1.0),
    }


def product(left, right):
    return jnp.einsum("bij,bjk->bik", left, right, precision=lax.Precision.HIGHEST)


def solve_tiles(a_diag, e_diag, resid_c, resid_f, inv_d, vec_left, back_left, eig_left, inv_e, vec_right, back_right, eig_right):
    coupled = product(a_diag, inv_d)
    merged = product(resid_c - product(coupled, resid_f), inv_e)
    spectral = product(product(back_left, merged), vec_right)
    spectral = spectral / (eig_left[:, :, None] - eig_right[:, None, :])
    new_l = product(product(vec_left, spectral), back_right)
    new_r = product(inv_d, resid_f + product(new_l, e_diag))
    return new_r, new_l


def reference(rhs_c, rhs_f, pencil_a, pencil_d, pencil_b, pencil_e, d_inverse, left_vectors, left_inverse, left_eigs, e_inverse, right_vectors, right_inverse, right_eigs):
    blocks = ORDER // TILE
    highest = lax.Precision.HIGHEST

    def grid(field):
        return field.astype(jnp.float32).reshape(blocks, TILE, blocks, TILE)

    current_c = grid(rhs_c)
    current_f = grid(rhs_f)
    tiles_a = grid(pencil_a)
    tiles_d = grid(pencil_d)
    tiles_b = grid(pencil_b)
    tiles_e = grid(pencil_e)
    inv_d = d_inverse.reshape(blocks, TILE, TILE)
    vec_left = left_vectors.reshape(blocks, TILE, TILE)
    back_left = left_inverse.reshape(blocks, TILE, TILE)
    eig_left = left_eigs.reshape(blocks, TILE)
    inv_e = e_inverse.reshape(blocks, TILE, TILE)
    vec_right = right_vectors.reshape(blocks, TILE, TILE)
    back_right = right_inverse.reshape(blocks, TILE, TILE)
    eig_right = right_eigs.reshape(blocks, TILE)
    out_r = jnp.zeros_like(current_c)
    out_l = jnp.zeros_like(current_c)
    count = jnp.arange(blocks, dtype=jnp.int32)
    for step in range(STEPS):
        offset = 1 - step
        front_rows = count + offset
        col_valid = (front_rows >= 0) & (front_rows < blocks)
        rows_clip = jnp.clip(front_rows, 0, blocks - 1).astype(jnp.int32)
        front_cols = count - offset
        row_valid = (front_cols >= 0) & (front_cols < blocks)
        cols_clip = jnp.clip(front_cols, 0, blocks - 1).astype(jnp.int32)
        resid_c = current_c[rows_clip, :, count, :]
        resid_f = current_f[rows_clip, :, count, :]
        a_diag = tiles_a[rows_clip, :, rows_clip, :]
        e_diag = tiles_e[count, :, count, :]
        new_r, new_l = solve_tiles(a_diag, e_diag, resid_c, resid_f, inv_d[rows_clip], vec_left[rows_clip], back_left[rows_clip], eig_left[rows_clip], inv_e, vec_right, back_right, eig_right)
        new_r = jnp.where(col_valid[:, None, None], new_r, 0.0)
        new_l = jnp.where(col_valid[:, None, None], new_l, 0.0)
        panel_a = tiles_a[:, :, rows_clip, :]
        panel_d = tiles_d[:, :, rows_clip, :]
        mask_a = (count[:, None] < front_rows[None, :]) & col_valid[None, :]
        term_c = jnp.einsum("kpjq,jqs->kpjs", panel_a, new_r, precision=highest)
        term_f = jnp.einsum("kpjq,jqs->kpjs", panel_d, new_r, precision=highest)
        row_l = jnp.where(row_valid[:, None, None], new_l[cols_clip], 0.0)
        panel_b = tiles_b[cols_clip]
        panel_e = tiles_e[cols_clip]
        mask_b = (count[None, :] > front_cols[:, None]) & row_valid[:, None]
        gain_c = jnp.einsum("ipq,iqls->ipls", row_l, panel_b, precision=highest)
        gain_f = jnp.einsum("ipq,iqls->ipls", row_l, panel_e, precision=highest)
        wide_a = mask_a[:, None, :, None]
        wide_b = mask_b[:, None, :, None]
        current_c = current_c - jnp.where(wide_a, term_c, 0.0) + jnp.where(wide_b, gain_c, 0.0)
        current_f = current_f - jnp.where(wide_a, term_f, 0.0) + jnp.where(wide_b, gain_f, 0.0)
        out_r = out_r.at[rows_clip, :, count, :].add(new_r)
        out_l = out_l.at[rows_clip, :, count, :].add(new_l)
    shape = (RT, N_ROW * TILE, CT, N_COL * TILE)
    return current_c.reshape(shape), current_f.reshape(shape), out_r.reshape(shape), out_l.reshape(shape)
```

```python
import functools
import math

import jax
import jax.numpy as jnp
from jax import lax
from jax.experimental import pallas as pl
from jax.experimental.pallas import tpu as pltpu
from jax.sharding import PartitionSpec as P

TILE = 128
MESH = pl.DeviceIdType.MESH
EARLY_SENDS = {"ahead": 2, "level": 7, "behind": 12}
EARLY_RELAYS = {"ahead": 0, "level": 1, "behind": 4}
LAG = 16
WRAP_LAG = 9
HANDLE_AT = {"ahead": 6, "level": 9, "behind": 13}
HANDLE_HOP = 3
IN_FLIGHT = 3


def heights(rows_dev, cols_dev, count_rows, count_cols):
    return [min(rows_dev, (b * count_cols + count_cols - 1) // count_rows + 1) for b in range(cols_dev)]


def split(value):
    hi = value.astype(jnp.bfloat16)
    return hi, (value - hi.astype(jnp.float32)).astype(jnp.bfloat16)


def dot(left, right):
    return jnp.dot(left, right, preferred_element_type=jnp.float32)


def product(left, right):
    left_hi, left_lo = split(left)
    right_hi, right_lo = split(right)
    return dot(
        jnp.concatenate([left_hi, left_lo, left_hi], axis=1), jnp.concatenate([right_hi, right_hi, right_lo], axis=0)
    )


def half_product(exact, value):
    return dot(jnp.concatenate([exact, exact], axis=1), jnp.concatenate(split(value), axis=0))


def product_half(value, exact):
    return dot(jnp.concatenate(split(value), axis=1), jnp.concatenate([exact, exact], axis=0))


def kernel(
    count_rows, count_cols, unit, tall,
    c_in, f_in, a_in, d_in, b_in, e_in, dinv_in, vec_left_in, back_left_in, eig_left_ref, inv_e_in, vec_right_in, back_right_in, eig_right_ref,
    c_ref, f_ref, r_out, l_out,
    a_ref, d_ref, b_ref, e_ref, ad_buf, be_buf, r_buf, l_buf, r_cat, l_cat,
    front_c, front_f, inv_d, vec_left, back_left, inv_e, vec_right, back_right, a_diag, e_diag, ad_right, be_up,
    ad_send, ad_recv, be_send, be_recv, r_send, r_recv, l_send, l_own_send, l_recv, small_send, small_recv, load_sem,
):
    rows_dev, cols_dev = c_ref.shape[:2]
    blocks = rows_dev * count_rows
    row, col = lax.axis_index("row"), lax.axis_index("col")
    pieces = [n // unit for n in tall]
    offsets = [sum(pieces[:b]) for b in range(cols_dev)]
    chunks = sum(pieces)

    def where_is(n):
        b = sum((n >= offset).astype(jnp.int32) for offset in offsets[1:]) if cols_dev > 1 else jnp.int32(0)
        return b, n - pick(b, offsets)

    def pick(b, values):
        out = jnp.int32(values[0])
        for k in range(1, len(values)):
            out = jnp.where(b == k, values[k], out)
        return out

    def chunk_of(b, q):
        return pick(b, offsets) + jnp.minimum(q, pick(b, pieces) - 1)

    phase = lax.rem(col - row + count_rows, count_rows)
    ahead, level, behind = phase == count_rows - 1, phase == 0, phase == 1
    active = ahead | level | behind
    feeder = (phase == 1) | (phase == 2)
    front = jnp.where(ahead, 1, -phase)
    mine, valid = [], []
    for b in range(cols_dev):
        i = b * count_cols + col + front
        valid.append(active & (i >= 0) & (i < blocks))
        mine.append(jnp.clip(i, 0, blocks - 1) // count_rows)

    partner_row = row + 1 - 2 * lax.rem(row, 2)
    cross_row = lax.rem(row + jnp.where(lax.rem(row, 2) == 0, count_rows - 1, 1), count_rows)
    partner_col = col + 1 - 2 * lax.rem(col, 2)
    relay_col = lax.rem(col + jnp.where(lax.rem(col, 2) == 0, 2, count_cols - 2), count_cols)
    even_col = lax.rem(col, 2) == 0
    left_col, right_col = lax.rem(col + count_cols - 1, count_cols), lax.rem(col + 1, count_cols)
    up_row, down_row = lax.rem(row + count_rows - 1, count_rows), lax.rem(row + 1, count_rows)

    def phase_of(r, c):
        return lax.rem(c - r + count_rows, count_rows)

    def is_active(r, c):
        p = phase_of(r, c)
        return (p == count_rows - 1) | (p == 0) | (p == 1)

    def remote(src, dst, send, recv, r, c):
        return pltpu.make_async_remote_copy(
            src_ref=src, dst_ref=dst, send_sem=send, recv_sem=recv, device_id=(r, c), device_id_type=MESH
        )

    def local(src, dst, sem):
        return pltpu.make_async_copy(src, dst, sem)

    solve_loads = []
    for b in range(cols_dev):
        for k, (src, dst) in enumerate([(c_in, front_c), (f_in, front_f)]):
            solve_loads.append(local(src.at[mine[b], b], dst.at[b], load_sem.at[k]))
        for k, (src, dst) in enumerate([(dinv_in, inv_d), (vec_left_in, vec_left), (back_left_in, back_left)]):
            solve_loads.append(local(src.at[mine[b]], dst.at[b], load_sem.at[2 + k]))
    fixed_loads = [
        local(src, dst, load_sem.at[5 + k])
        for k, (src, dst) in enumerate([(inv_e_in, inv_e), (vec_right_in, vec_right), (back_right_in, back_right)])
    ]
    for copy in solve_loads + fixed_loads:
        copy.start()

    barrier = pltpu.get_barrier_semaphore()
    for k in range(1, count_rows):
        pl.semaphore_signal(barrier, inc=1, device_id=(lax.rem(row + k, count_rows), col), device_id_type=MESH)
    for k in range(1, count_cols):
        pl.semaphore_signal(barrier, inc=1, device_id=(row, lax.rem(col + k, count_cols)), device_id_type=MESH)
    pl.semaphore_wait(barrier, count_rows + count_cols - 2)

    @pl.when(level)
    def _():
        for b in range(cols_dev):
            local(a_in.at[mine[b], b], a_diag.at[b], small_recv.at[0]).start()
            local(e_in.at[mine[b], b], e_diag.at[b], small_recv.at[1]).start()
        for b in range(cols_dev):
            at = b - (col == 0).astype(jnp.int32)

            @pl.when(at >= 0)
            def _():
                remote(a_in.at[mine[b], b], a_diag.at[jnp.maximum(at, 0)], small_send.at[0], small_recv.at[0], row, left_col).start()

            to = b + (col == count_cols - 1).astype(jnp.int32)

            @pl.when(to < cols_dev)
            def _():
                remote(a_in.at[mine[b], b], a_diag.at[jnp.minimum(to, cols_dev - 1)], small_send.at[1], small_recv.at[0], row, right_col).start()

            remote(e_in.at[mine[b], b], e_diag.at[b], small_send.at[2], small_recv.at[1], down_row, col).start()
            remote(e_in.at[mine[b], b], e_diag.at[b], small_send.at[3], small_recv.at[1], up_row, col).start()

    @pl.when(feeder)
    def _():
        for b in range(cols_dev):
            at = b - (col == 0).astype(jnp.int32)

            @pl.when(at >= 0)
            def _():
                for k, src in enumerate((a_in, d_in)):
                    remote(src.at[mine[b], b], ad_right.at[jnp.maximum(at, 0), k], small_send.at[4], small_recv.at[2], row, left_col).start()

            for k, src in enumerate((b_in, e_in)):
                remote(src.at[mine[b], b], be_up.at[b, k], small_send.at[5], small_recv.at[3], down_row, col).start()

    def swap(n):
        b, q = where_is(n)
        for k, src in enumerate((a_in, d_in)):
            remote(src.at[pl.ds(q * unit, unit), b], ad_buf.at[0, n, k], ad_send.at[0, n], ad_recv.at[0, n], row, partner_col).start()

    def cross(n):
        b, q = where_is(n)
        for k, src in enumerate((b_in, e_in)):
            remote(src.at[pl.ds(q * unit, unit), b], be_buf.at[1, n, k], be_send.at[1, n], be_recv.at[1, n], cross_row, col).start()

    def near(n):
        b, q = where_is(n)
        for k, src in enumerate((b_in, e_in)):
            remote(src.at[pl.ds(q * unit, unit), b], be_buf.at[0, n, k], be_send.at[0, n], be_recv.at[0, n], partner_row, col).start()

    def whole_ad(side, n):
        return remote(ad_buf.at[side, n], ad_buf.at[side, n], ad_send.at[side, n], ad_recv.at[side, n], row, partner_col)

    def whole_be(side, n):
        return remote(be_buf.at[side, n], be_buf.at[side, n], be_send.at[side, n], be_recv.at[side, n], partner_row, col)

    def relay_sent(n):
        b, _ = where_is(n)
        skip = ((col == count_cols - 2) & (b == cols_dev - 1)) | ((col == 1) & (b == 0))
        return jnp.logical_not(skip)

    def relay(n):
        whole_ad(0, n).wait_recv()

        @pl.when(relay_sent(n))
        def _():
            remote(ad_buf.at[0, n], ad_buf.at[1, n], ad_send.at[1, n], ad_recv.at[1, n], row, relay_col).start()

    def loop(lo, hi, body):
        lax.fori_loop(lo, hi, lambda n, _: (body(n), 0)[1], 0)

    early = jnp.int32(min(IN_FLIGHT, chunks))
    sent = jnp.int32(0)
    for name, flag in (("ahead", ahead), ("level", level), ("behind", behind)):
        early = jnp.where(flag, min(EARLY_SENDS[name], chunks), early)
        sent = jnp.where(flag, min(EARLY_RELAYS[name], chunks), sent)

    wraps = (col == 1) | (col == count_cols - 2)
    sent = jnp.where(wraps, 0, sent)
    loop(0, early, swap)
    loop(0, early, cross)
    loop(0, chunks, near)
    big_loads = [
        local(src, dst, load_sem.at[8 + k])
        for k, (src, dst) in enumerate([(a_in, a_ref), (d_in, d_ref), (b_in, b_ref), (e_in, e_ref), (c_in, c_ref), (f_in, f_ref)])
    ]
    for copy in big_loads:
        copy.start()
    loop(0, sent, relay)

    for k, dst in enumerate((front_c, front_f, inv_d, vec_left, back_left)):
        local(dst, dst, load_sem.at[k]).wait()
    for copy in fixed_loads:
        copy.wait()

    at_last = (col == count_cols - 1).astype(jnp.int32)

    def wait_tiles(ref, sem, short):
        @pl.when(jnp.logical_not(short))
        def _():
            local(ref, ref, sem).wait()

        if cols_dev > 1:

            @pl.when(short)
            def _():
                part = ref.at[pl.ds(0, cols_dev - 1)]
                local(part, part, sem).wait()

    @pl.when(active)
    def _():
        short = (ahead & (col == count_cols - 1)) | (behind & (col == 0))
        wait_tiles(a_diag, small_recv.at[0], short)
        local(e_diag, e_diag, small_recv.at[1]).wait()

    def got_l(c, b):
        back = (c < 0).astype(jnp.int32)
        slot = b - back
        tile = l_buf[lax.rem(c + count_cols, count_cols), jnp.maximum(slot, 0)]
        return jnp.where(slot >= 0, tile, 0.0)

    def wait_r(r):
        remote(r_buf.at[r], r_buf.at[r], r_send.at[0], r_recv.at[r], row, col).wait_recv()

    def wait_l(c):
        remote(l_buf.at[c], l_buf.at[c], l_send.at[0], l_recv.at[c], row, col).wait_recv()

    def direct(src, dst):
        p = phase_of(row, src)
        return (lax.rem(src, 2) == 1) & (dst == lax.rem(src + 1, count_cols)) & ((p == count_rows - 1) | (p == 0))

    def own_routes():
        order = [k for n in range(1, count_cols // 4 + 1) for k in dict.fromkeys((n, count_cols // 2 - n))]
        routes = [(direct(col, right_col), right_col)] + [(None, lax.rem(col + 2 * k, count_cols)) for k in order]
        return routes

    def across(src):
        return (src != col) & (lax.rem(src + col, 2) == 0) & jnp.logical_not(direct(src, partner_col))

    def maybe(when, run):
        return run() if when is None else pl.when(when)(run)

    def send_l(src):
        remote(l_buf.at[src], l_buf.at[src], l_send.at[src], l_recv.at[src], row, partner_col).start()

    def send_own_l():
        send_l(col)
        for k, (when, to) in enumerate(own_routes()):
            maybe(when, lambda: remote(l_buf.at[col], l_buf.at[col], l_own_send.at[k], l_recv.at[col], row, to).start())

    def handle(src):
        wait_l(src)
        pl.when(across(src))(lambda: send_l(src))

    def absorb(ad, be, right, left):
        for b in range(cols_dev):
            a_tile, d_tile = ad(b)
            b_tile, e_tile = be(b)
            value_r, value_l = right(b), left(b)
            front_c[b] = front_c[b] - half_product(a_tile, value_r) + product_half(value_l, b_tile)
            front_f[b] = front_f[b] - half_product(d_tile, value_r) + product_half(value_l, e_tile)

    row_ahead, row_level = lax.rem(col + 1, count_rows), lax.rem(col, count_rows)
    col_first = jnp.where(level, col - 1, col - 2)

    @pl.when(level | behind)
    def _():
        wait_tiles(ad_right, small_recv.at[2], col == count_cols - 1)
        local(be_up, be_up, small_recv.at[3]).wait()
        wait_r(row_ahead)
        handle(lax.rem(col_first + count_cols, count_cols))

        def right_tiles(b):
            tiles = ad_right[b, 0], ad_right[b, 1]
            if b < cols_dev - 1:
                return tiles
            return tuple(jnp.where(col == count_cols - 1, jnp.zeros_like(tile), tile) for tile in tiles)

        absorb(right_tiles, lambda b: (be_up[b, 0], be_up[b, 1]), lambda b: r_buf[row_ahead, b], lambda b: got_l(col_first, b))

    @pl.when(behind)
    def _():
        for copy in big_loads[:4]:
            copy.wait()
        wait_r(row_level)
        handle(left_col)
        absorb(
            lambda b: (a_ref[mine[b], b], d_ref[mine[b], b]),
            lambda b: (b_ref[mine[b], b], e_ref[mine[b], b]),
            lambda b: r_buf[row_level, b],
            lambda b: got_l(col - 1, b),
        )

    @pl.when(active)
    def _():
        span = range(cols_dev)
        coupled = [half_product(a_diag[b], inv_d[b]) for b in span]
        merged = [front_c[b] - product(coupled[b], front_f[b]) for b in span]
        merged = [product(merged[b], inv_e[b]) for b in span]
        spectral = [product(back_left[b], merged[b]) for b in span]
        spectral = [product(spectral[b], vec_right[b]) for b in span]
        for b in span:
            eig = jnp.broadcast_to(eig_left_ref[pl.ds(mine[b], 1), :], (TILE, TILE)).T
            spectral[b] = spectral[b] / (eig - eig_right_ref[pl.ds(b, 1), :])
        new_l = [product(vec_left[b], spectral[b]) for b in span]
        new_l = [product(new_l[b], back_right[b]) for b in span]
        for b in span:
            l_buf[col, b] = jnp.where(valid[b], new_l[b], 0.0)
        summed = [front_f[b] + product_half(new_l[b], e_diag[b]) for b in span]
        for b in span:
            r_buf[row, b] = jnp.where(valid[b], product(inv_d[b], summed[b]), 0.0)

        for k in range(1, count_rows):
            to = lax.rem(row + count_rows - k, count_rows)
            remote(r_buf.at[row], r_buf.at[row], r_send.at[k], r_recv.at[row], to, col).start()
        send_own_l()

    loop(early, chunks, cross)

    lag = min(LAG, chunks - 1)

    def handled(src):
        before = ((level | behind) & (src == left_col)) | (behind & (src == lax.rem(col + count_cols - 2, count_cols)))
        return before | (src == col) | jnp.logical_not(is_active(row, src))

    def handle_at(src):
        p = phase_of(row, src)
        base = jnp.where(p == count_rows - 1, HANDLE_AT["ahead"], jnp.where(p == 0, HANDLE_AT["level"], HANDLE_AT["behind"]))
        return jnp.minimum(base + jnp.where(lax.rem(src + col, 2) == 0, 0, HANDLE_HOP), lag)

    def collect():
        for offset in range(1, -2, -1):
            src = lax.rem(col + offset + count_rows, count_rows)
            taken = ((level | behind) & (src == row_ahead)) | (behind & (src == row_level)) | (src == row)

            @pl.when(jnp.logical_not(taken))
            def _():
                wait_r(src)

        for b in range(cols_dev):
            for k, offset in enumerate((1, 0, -1)):
                hi, lo = split(r_buf[lax.rem(col + offset + count_rows, count_rows), b])
                r_cat[b, k * TILE : (k + 1) * TILE, :TILE] = hi
                r_cat[b, k * TILE : (k + 1) * TILE, TILE:] = lo

        def gather(a):
            for k, offset in enumerate((1, 0, -1)):
                m = a * count_rows + row - offset
                at = jnp.clip(m, 0, blocks - 1)
                tile = l_buf[lax.rem(at, count_cols), at // count_cols]
                hi, lo = split(jnp.where((m >= 0) & (m < blocks), tile, 0.0))
                l_cat[a, :TILE, k * TILE : (k + 1) * TILE] = hi
                l_cat[a, TILE:, k * TILE : (k + 1) * TILE] = lo

        loop(0, rows_dev, gather)

        @pl.when(jnp.logical_not(behind))
        def _():
            for copy in big_loads[:4]:
                copy.wait()

        for copy in big_loads[4:]:
            copy.wait()

    right_side, left_side = lax.rem(col, 2), 1 - lax.rem(col, 2)
    up_side, down_side = 1 - lax.rem(row, 2), lax.rem(row, 2)
    first_relay = jnp.where(col == count_cols - 1, offsets[1] if cols_dev > 1 else chunks, 0)

    def right_chunk(b, q):
        slot = jnp.minimum(b + at_last, cols_dev - 1)
        return chunk_of(slot, q)

    def left_chunk(b, q):
        slot = jnp.maximum(b - (col == 0).astype(jnp.int32), 0)
        return chunk_of(slot, q)

    def need(m):
        b, q = where_is(m)
        at = jnp.where(even_col, left_chunk(b, q), right_chunk(b, q))
        return jnp.where((col == count_cols - 1) & (b == cols_dev - 1), chunks - 1, at)

    def be_tile(side, which, b, a, height):
        at = jnp.clip(a, 0, height - 1)
        return be_buf[side, pick(b, offsets) + at // unit, which, lax.rem(at, unit)]

    def update(m):
        b, q = where_is(m)
        height = pick(b, tall)
        whole_be(0, m).wait_recv()
        lo = jnp.where(m == 0, 0, jnp.minimum(m + 1, chunks))
        loop(lo, jnp.minimum(m + 2, chunks), lambda n: whole_be(1, n).wait_recv())
        lo = jnp.where(m == 0, first_relay, need(jnp.maximum(m - 1, 0)) + 1)
        loop(lo, need(m) + 1, lambda n: whole_ad(1, n).wait_recv())
        at_right, at_left = right_chunk(b, q), left_chunk(b, q)
        j = b * count_cols + col
        for t in range(unit):
            a = q * unit + t
            i = a * count_rows + row
            up_a, down_a = a - (row == 0).astype(jnp.int32), a + (row == count_rows - 1).astype(jnp.int32)

            def apply(near_edge):
                def masked(tile, keep):
                    return jnp.where(keep, tile, jnp.zeros_like(tile)) if near_edge else tile

                def wide(which, own):
                    return jnp.concatenate(
                        [
                            ad_buf[right_side, at_right, which, t],
                            masked(own[a, b], i < j),
                            masked(ad_buf[left_side, at_left, which, t], i < j - 1),
                        ],
                        axis=1,
                    )

                def high(which, own):
                    return jnp.concatenate(
                        [
                            be_tile(up_side, which, b, up_a, height),
                            masked(own[a, b], i < j),
                            masked(be_tile(down_side, which, b, down_a, height), i < j - 1),
                        ],
                        axis=0,
                    )

                first = dot(jnp.concatenate([wide(0, a_ref), wide(1, d_ref)], axis=0), r_cat[b])
                second = dot(l_cat[a], jnp.concatenate([high(0, b_ref), high(1, e_ref)], axis=1))
                c_ref[a, b] = c_ref[a, b] - (first[:TILE, :TILE] + first[:TILE, TILE:]) + (second[:TILE, :TILE] + second[TILE:, :TILE])
                f_ref[a, b] = f_ref[a, b] - (first[TILE:, :TILE] + first[TILE:, TILE:]) + (second[:TILE, TILE:] + second[TILE:, TILE:])

            pl.when(i < j - 1)(lambda: apply(False))
            pl.when((i == j) | (i == j - 1))(lambda: apply(True))

    def done_by(n):
        return jnp.clip((n - lag + 1) * 3, 0, jnp.maximum(n - 1, 0))

    def wrapped_by(n):
        return jnp.where(wraps, jnp.clip((n - min(WRAP_LAG, chunks - 1) + 1) * 2, 0, jnp.maximum(n + 1, 0)), 0)

    def main(n):
        loop(jnp.maximum(early, jnp.where(n == 0, 0, n + IN_FLIGHT)), jnp.minimum(n + IN_FLIGHT + 1, chunks), swap)
        pl.when((n >= sent) & jnp.logical_not(wraps))(lambda: relay(n))
        loop(wrapped_by(n - 1), wrapped_by(n), relay)
        loop(0, count_cols, lambda src: pl.when((n == handle_at(src)) & jnp.logical_not(handled(src)))(lambda: handle(src)))
        pl.when(n == lag)(collect)
        loop(done_by(n - 1), done_by(n), update)

    loop(0, chunks, main)
    loop(wrapped_by(chunks - 1), jnp.where(wraps, chunks, 0), relay)
    loop(done_by(chunks - 1), chunks, update)

    copies = [local(r_buf.at[row], r_out, load_sem.at[14]), local(l_buf.at[col], l_out, load_sem.at[15])]
    for copy in copies:
        copy.start()

    def drain(n):
        whole_ad(0, n).wait_send()
        pl.when(relay_sent(n))(lambda: whole_ad(1, n).wait_send())
        whole_be(0, n).wait_send()
        whole_be(1, n).wait_send()

    loop(0, chunks, drain)

    def wait_sent(ref, sem):
        remote(ref, ref, sem, r_recv.at[0], row, col).wait_send()

    def wait_tiles_sent(ref, sem, short):
        pl.when(jnp.logical_not(short))(lambda: wait_sent(ref, sem))
        if cols_dev > 1:
            pl.when(short)(lambda: wait_sent(ref.at[pl.ds(0, cols_dev - 1)], sem))

    @pl.when(level)
    def _():
        wait_tiles_sent(a_diag, small_send.at[0], col == 0)
        wait_tiles_sent(a_diag, small_send.at[1], col == count_cols - 1)
        wait_sent(e_diag, small_send.at[2])
        wait_sent(e_diag, small_send.at[3])

    @pl.when(feeder)
    def _():
        wait_tiles_sent(ad_right, small_send.at[4], col == 0)
        wait_sent(be_up, small_send.at[5])

    @pl.when(active)
    def _():
        for k in range(1, count_rows):
            wait_sent(r_buf.at[row], r_send.at[k])

        for k, (when, _) in enumerate(own_routes()):
            maybe(when, lambda: wait_sent(l_buf.at[col], l_own_send.at[k]))

    def drain_l(src):
        pl.when(is_active(row, src) & ((src == col) | across(src)))(lambda: wait_sent(l_buf.at[src], l_send.at[src]))

    loop(0, count_cols, drain_l)

    for copy in copies:
        copy.wait()


def body(*args):
    count_rows = lax.axis_size("row")
    count_cols = lax.axis_size("col")
    row, col = lax.axis_index("row"), lax.axis_index("col")
    wide = [x.transpose(0, 2, 1, 3) for x in args[:6]]
    rows_dev, cols_dev = wide[0].shape[:2]
    blocks = rows_dev * count_rows
    tall = heights(rows_dev, cols_dev, count_rows, count_cols)
    unit = math.gcd(*tall)
    chunks = sum(tall) // unit
    anywhere, inside = pl.BlockSpec(memory_space=pl.ANY), pl.BlockSpec(memory_space=pltpu.VMEM)
    whole, few = (rows_dev, cols_dev, TILE, TILE), (cols_dev, TILE, TILE)
    f32, bf16 = jnp.float32, jnp.bfloat16
    dma = pltpu.SemaphoreType.DMA
    new_c, new_f, new_r, new_l = pl.pallas_call(
        functools.partial(kernel, count_rows, count_cols, unit, tall),
        in_specs=[anywhere] * 9 + [inside] + [anywhere] * 3 + [inside],
        out_specs=[inside, inside, anywhere, anywhere],
        out_shape=[jax.ShapeDtypeStruct(whole, f32)] * 2 + [jax.ShapeDtypeStruct(few, f32)] * 2,
        scratch_shapes=[pltpu.VMEM(whole, bf16)] * 4
        + [pltpu.VMEM((2, chunks, 2, unit, TILE, TILE), bf16)] * 2
        + [
            pltpu.VMEM((count_rows,) + few, f32),
            pltpu.VMEM((count_cols,) + few, f32),
            pltpu.VMEM((cols_dev, 3 * TILE, 2 * TILE), bf16),
            pltpu.VMEM((rows_dev, 2 * TILE, 3 * TILE), bf16),
        ]
        + [pltpu.VMEM(few, f32)] * 8
        + [pltpu.VMEM(few, bf16)] * 2
        + [pltpu.VMEM((cols_dev, 2, TILE, TILE), bf16)] * 2
        + [dma((2, chunks))] * 4
        + [dma((count_rows,)), dma((count_rows,)), dma((count_cols,)), dma((count_cols,)), dma((count_cols,)), dma((6,)), dma((4,)), dma((16,))],
        compiler_params=pltpu.CompilerParams(collective_id=0, has_side_effects=True, vmem_limit_bytes=60 * 1024 * 1024),
        name="fronts",
    )(*wide, *args[6:])

    phase = (col - row) % count_rows
    front = jnp.where(phase == count_rows - 1, 1, -phase)
    active = (phase == count_rows - 1) | (phase <= 1)
    at = jnp.arange(cols_dev, dtype=jnp.int32) * count_cols + col + front
    i = jnp.arange(rows_dev, dtype=jnp.int32)[:, None] * count_rows + row
    here = (active & (i == at[None, :]))[:, :, None, None]
    out_r = jnp.where(here, new_r[None], 0.0)
    out_l = jnp.where(here, new_l[None], 0.0)
    return tuple(x.transpose(0, 2, 1, 3) for x in (new_c, new_f, out_r, out_l))


def solution(mesh):
    grid = P(None, "row", None, "col")
    left, right = P(None, "row", None), P(None, "col", None)
    in_specs = (grid,) * 6 + (left,) * 3 + (P(None, "row"),) + (right,) * 3 + (P(None, "col"),)
    return jax.shard_map(body, mesh=mesh, in_specs=in_specs, out_specs=(grid,) * 4, check_vma=False)
```

```python
import functools
import math

import jax
import jax.numpy as jnp
from jax import lax
from jax.experimental import pallas as pl
from jax.experimental.pallas import tpu as pltpu
from jax.sharding import PartitionSpec as P

TILE = 128
MESH = pl.DeviceIdType.MESH
EARLY_SENDS = {"ahead": 2, "level": 7, "behind": 12}
EARLY_RELAYS = {"ahead": 0, "level": 1, "behind": 4}
LAG = 16
WRAP_LAG = 9
HANDLE_AT = {"ahead": 6, "level": 9, "behind": 13}
HANDLE_HOP = 3
IN_FLIGHT = 5


def heights(rows_dev, cols_dev, count_rows, count_cols):
    return [min(rows_dev, (b * count_cols + count_cols - 1) // count_rows + 1) for b in range(cols_dev)]


def split(value):
    hi = value.astype(jnp.bfloat16)
    return hi, (value - hi.astype(jnp.float32)).astype(jnp.bfloat16)


def dot(left, right):
    return jnp.dot(left, right, preferred_element_type=jnp.float32)


def product(left, right):
    left_hi, left_lo = split(left)
    right_hi, right_lo = split(right)
    return dot(
        jnp.concatenate([left_hi, left_lo, left_hi], axis=1), jnp.concatenate([right_hi, right_hi, right_lo], axis=0)
    )


def half_product(exact, value):
    return dot(jnp.concatenate([exact, exact], axis=1), jnp.concatenate(split(value), axis=0))


def product_half(value, exact):
    return dot(jnp.concatenate(split(value), axis=1), jnp.concatenate([exact, exact], axis=0))


def kernel(
    count_rows, count_cols, unit, tall,
    c_in, f_in, a_in, d_in, b_in, e_in, dinv_in, vec_left_in, back_left_in, eig_left_ref, inv_e_in, vec_right_in, back_right_in, eig_right_ref,
    c_ref, f_ref, r_out, l_out,
    a_ref, d_ref, b_ref, e_ref, ad_buf, be_buf, r_buf, l_buf, r_cat, l_cat,
    front_c, front_f, inv_d, vec_left, back_left, inv_e, vec_right, back_right, a_diag, e_diag, ad_right, be_up,
    ad_send, ad_recv, be_send, be_recv, r_send, r_recv, l_send, l_own_send, l_recv, small_send, small_recv, load_sem,
):
    rows_dev, cols_dev = c_ref.shape[:2]
    blocks = rows_dev * count_rows
    row, col = lax.axis_index("row"), lax.axis_index("col")
    pieces = [n // unit for n in tall]
    offsets = [sum(pieces[:b]) for b in range(cols_dev)]
    chunks = sum(pieces)

    def where_is(n):
        b = sum((n >= offset).astype(jnp.int32) for offset in offsets[1:]) if cols_dev > 1 else jnp.int32(0)
        return b, n - pick(b, offsets)

    def pick(b, values):
        out = jnp.int32(values[0])
        for k in range(1, len(values)):
            out = jnp.where(b == k, values[k], out)
        return out

    def chunk_of(b, q):
        return pick(b, offsets) + jnp.minimum(q, pick(b, pieces) - 1)

    phase = lax.rem(col - row + count_rows, count_rows)
    ahead, level, behind = phase == count_rows - 1, phase == 0, phase == 1
    active = ahead | level | behind
    feeder = (phase == 1) | (phase == 2)
    front = jnp.where(ahead, 1, -phase)
    mine, valid = [], []
    for b in range(cols_dev):
        i = b * count_cols + col + front
        valid.append(active & (i >= 0) & (i < blocks))
        mine.append(jnp.clip(i, 0, blocks - 1) // count_rows)

    partner_row = row + 1 - 2 * lax.rem(row, 2)
    cross_row = lax.rem(row + jnp.where(lax.rem(row, 2) == 0, count_rows - 1, 1), count_rows)
    partner_col = col + 1 - 2 * lax.rem(col, 2)
    relay_col = lax.rem(col + jnp.where(lax.rem(col, 2) == 0, 2, count_cols - 2), count_cols)
    even_col = lax.rem(col, 2) == 0
    left_col, right_col = lax.rem(col + count_cols - 1, count_cols), lax.rem(col + 1, count_cols)
    up_row, down_row = lax.rem(row + count_rows - 1, count_rows), lax.rem(row + 1, count_rows)

    def phase_of(r, c):
        return lax.rem(c - r + count_rows, count_rows)

    def is_active(r, c):
        p = phase_of(r, c)
        return (p == count_rows - 1) | (p == 0) | (p == 1)

    def remote(src, dst, send, recv, r, c):
        return pltpu.make_async_remote_copy(
            src_ref=src, dst_ref=dst, send_sem=send, recv_sem=recv, device_id=(r, c), device_id_type=MESH
        )

    def local(src, dst, sem):
        return pltpu.make_async_copy(src, dst, sem)

    solve_loads = []
    for b in range(cols_dev):
        for k, (src, dst) in enumerate([(c_in, front_c), (f_in, front_f)]):
            solve_loads.append(local(src.at[mine[b], b], dst.at[b], load_sem.at[k]))
        for k, (src, dst) in enumerate([(dinv_in, inv_d), (vec_left_in, vec_left), (back_left_in, back_left)]):
            solve_loads.append(local(src.at[mine[b]], dst.at[b], load_sem.at[2 + k]))
    fixed_loads = [
        local(src, dst, load_sem.at[5 + k])
        for k, (src, dst) in enumerate([(inv_e_in, inv_e), (vec_right_in, vec_right), (back_right_in, back_right)])
    ]
    for copy in solve_loads + fixed_loads:
        copy.start()

    barrier = pltpu.get_barrier_semaphore()
    for k in range(1, count_rows):
        pl.semaphore_signal(barrier, inc=1, device_id=(lax.rem(row + k, count_rows), col), device_id_type=MESH)
    for k in range(1, count_cols):
        pl.semaphore_signal(barrier, inc=1, device_id=(row, lax.rem(col + k, count_cols)), device_id_type=MESH)
    pl.semaphore_wait(barrier, count_rows + count_cols - 2)

    @pl.when(level)
    def _():
        for b in range(cols_dev):
            local(a_in.at[mine[b], b], a_diag.at[b], small_recv.at[0]).start()
            local(e_in.at[mine[b], b], e_diag.at[b], small_recv.at[1]).start()
        for b in range(cols_dev):
            at = b - (col == 0).astype(jnp.int32)

            @pl.when(at >= 0)
            def _():
                remote(a_in.at[mine[b], b], a_diag.at[jnp.maximum(at, 0)], small_send.at[0], small_recv.at[0], row, left_col).start()

            to = b + (col == count_cols - 1).astype(jnp.int32)

            @pl.when(to < cols_dev)
            def _():
                remote(a_in.at[mine[b], b], a_diag.at[jnp.minimum(to, cols_dev - 1)], small_send.at[1], small_recv.at[0], row, right_col).start()

            remote(e_in.at[mine[b], b], e_diag.at[b], small_send.at[2], small_recv.at[1], down_row, col).start()
            remote(e_in.at[mine[b], b], e_diag.at[b], small_send.at[3], small_recv.at[1], up_row, col).start()

    @pl.when(feeder)
    def _():
        for b in range(cols_dev):
            at = b - (col == 0).astype(jnp.int32)

            @pl.when(at >= 0)
            def _():
                for k, src in enumerate((a_in, d_in)):
                    remote(src.at[mine[b], b], ad_right.at[jnp.maximum(at, 0), k], small_send.at[4], small_recv.at[2], row, left_col).start()

            for k, src in enumerate((b_in, e_in)):
                remote(src.at[mine[b], b], be_up.at[b, k], small_send.at[5], small_recv.at[3], down_row, col).start()

    def swap(n):
        b, q = where_is(n)
        for k, src in enumerate((a_in, d_in)):
            remote(src.at[pl.ds(q * unit, unit), b], ad_buf.at[0, n, k], ad_send.at[0, n], ad_recv.at[0, n], row, partner_col).start()

    def cross(n):
        b, q = where_is(n)
        for k, src in enumerate((b_in, e_in)):
            remote(src.at[pl.ds(q * unit, unit), b], be_buf.at[1, n, k], be_send.at[1, n], be_recv.at[1, n], cross_row, col).start()

    def near(n):
        b, q = where_is(n)
        for k, src in enumerate((b_in, e_in)):
            remote(src.at[pl.ds(q * unit, unit), b], be_buf.at[0, n, k], be_send.at[0, n], be_recv.at[0, n], partner_row, col).start()

    def whole_ad(side, n):
        return remote(ad_buf.at[side, n], ad_buf.at[side, n], ad_send.at[side, n], ad_recv.at[side, n], row, partner_col)

    def whole_be(side, n):
        return remote(be_buf.at[side, n], be_buf.at[side, n], be_send.at[side, n], be_recv.at[side, n], partner_row, col)

    def relay_sent(n):
        b, _ = where_is(n)
        skip = ((col == count_cols - 2) & (b == cols_dev - 1)) | ((col == 1) & (b == 0))
        return jnp.logical_not(skip)

    def relay(n):
        whole_ad(0, n).wait_recv()

        @pl.when(relay_sent(n))
        def _():
            remote(ad_buf.at[0, n], ad_buf.at[1, n], ad_send.at[1, n], ad_recv.at[1, n], row, relay_col).start()

    def loop(lo, hi, body):
        lax.fori_loop(lo, hi, lambda n, _: (body(n), 0)[1], 0)

    early = jnp.int32(min(IN_FLIGHT, chunks))
    sent = jnp.int32(0)
    for name, flag in (("ahead", ahead), ("level", level), ("behind", behind)):
        early = jnp.where(flag, min(EARLY_SENDS[name], chunks), early)
        sent = jnp.where(flag, min(EARLY_RELAYS[name], chunks), sent)

    wraps = (col == 1) | (col == count_cols - 2)
    sent = jnp.where(wraps, 0, sent)
    loop(0, early, swap)
    loop(0, early, cross)
    loop(0, chunks, near)
    big_loads = [
        local(src, dst, load_sem.at[8 + k])
        for k, (src, dst) in enumerate([(a_in, a_ref), (d_in, d_ref), (b_in, b_ref), (e_in, e_ref), (c_in, c_ref), (f_in, f_ref)])
    ]
    for copy in big_loads:
        copy.start()
    loop(0, sent, relay)

    for k, dst in enumerate((front_c, front_f, inv_d, vec_left, back_left)):
        local(dst, dst, load_sem.at[k]).wait()
    for copy in fixed_loads:
        copy.wait()

    at_last = (col == count_cols - 1).astype(jnp.int32)

    def wait_tiles(ref, sem, short):
        @pl.when(jnp.logical_not(short))
        def _():
            local(ref, ref, sem).wait()

        if cols_dev > 1:

            @pl.when(short)
            def _():
                part = ref.at[pl.ds(0, cols_dev - 1)]
                local(part, part, sem).wait()

    @pl.when(active)
    def _():
        short = (ahead & (col == count_cols - 1)) | (behind & (col == 0))
        wait_tiles(a_diag, small_recv.at[0], short)
        local(e_diag, e_diag, small_recv.at[1]).wait()

    def got_l(c, b):
        back = (c < 0).astype(jnp.int32)
        slot = b - back
        tile = l_buf[lax.rem(c + count_cols, count_cols), jnp.maximum(slot, 0)]
        return jnp.where(slot >= 0, tile, 0.0)

    def wait_r(r):
        remote(r_buf.at[r], r_buf.at[r], r_send.at[0], r_recv.at[r], row, col).wait_recv()

    def wait_l(c):
        remote(l_buf.at[c], l_buf.at[c], l_send.at[0], l_recv.at[c], row, col).wait_recv()

    def direct(src, dst):
        p = phase_of(row, src)
        return (lax.rem(src, 2) == 1) & (dst == lax.rem(src + 1, count_cols)) & ((p == count_rows - 1) | (p == 0))

    def own_routes():
        order = [k for n in range(1, count_cols // 4 + 1) for k in dict.fromkeys((n, count_cols // 2 - n))]
        routes = [(direct(col, right_col), right_col)] + [(None, lax.rem(col + 2 * k, count_cols)) for k in order]
        return routes

    def across(src):
        return (src != col) & (lax.rem(src + col, 2) == 0) & jnp.logical_not(direct(src, partner_col))

    def maybe(when, run):
        return run() if when is None else pl.when(when)(run)

    def send_l(src):
        remote(l_buf.at[src], l_buf.at[src], l_send.at[src], l_recv.at[src], row, partner_col).start()

    def send_own_l():
        send_l(col)
        for k, (when, to) in enumerate(own_routes()):
            maybe(when, lambda: remote(l_buf.at[col], l_buf.at[col], l_own_send.at[k], l_recv.at[col], row, to).start())

    def handle(src):
        wait_l(src)
        pl.when(across(src))(lambda: send_l(src))

    def absorb(ad, be, right, left):
        for b in range(cols_dev):
            a_tile, d_tile = ad(b)
            b_tile, e_tile = be(b)
            value_r, value_l = right(b), left(b)
            front_c[b] = front_c[b] - half_product(a_tile, value_r) + product_half(value_l, b_tile)
            front_f[b] = front_f[b] - half_product(d_tile, value_r) + product_half(value_l, e_tile)

    row_ahead, row_level = lax.rem(col + 1, count_rows), lax.rem(col, count_rows)
    col_first = jnp.where(level, col - 1, col - 2)

    @pl.when(level | behind)
    def _():
        wait_tiles(ad_right, small_recv.at[2], col == count_cols - 1)
        local(be_up, be_up, small_recv.at[3]).wait()
        wait_r(row_ahead)
        handle(lax.rem(col_first + count_cols, count_cols))

        def right_tiles(b):
            tiles = ad_right[b, 0], ad_right[b, 1]
            if b < cols_dev - 1:
                return tiles
            return tuple(jnp.where(col == count_cols - 1, jnp.zeros_like(tile), tile) for tile in tiles)

        absorb(right_tiles, lambda b: (be_up[b, 0], be_up[b, 1]), lambda b: r_buf[row_ahead, b], lambda b: got_l(col_first, b))

    @pl.when(behind)
    def _():
        for copy in big_loads[:4]:
            copy.wait()
        wait_r(row_level)
        handle(left_col)
        absorb(
            lambda b: (a_ref[mine[b], b], d_ref[mine[b], b]),
            lambda b: (b_ref[mine[b], b], e_ref[mine[b], b]),
            lambda b: r_buf[row_level, b],
            lambda b: got_l(col - 1, b),
        )

    @pl.when(active)
    def _():
        span = range(cols_dev)
        coupled = [half_product(a_diag[b], inv_d[b]) for b in span]
        merged = [front_c[b] - product(coupled[b], front_f[b]) for b in span]
        merged = [product(merged[b], inv_e[b]) for b in span]
        spectral = [product(back_left[b], merged[b]) for b in span]
        spectral = [product(spectral[b], vec_right[b]) for b in span]
        for b in span:
            eig = jnp.broadcast_to(eig_left_ref[pl.ds(mine[b], 1), :], (TILE, TILE)).T
            spectral[b] = spectral[b] / (eig - eig_right_ref[pl.ds(b, 1), :])
        new_l = [product(vec_left[b], spectral[b]) for b in span]
        new_l = [product(new_l[b], back_right[b]) for b in span]
        for b in span:
            l_buf[col, b] = jnp.where(valid[b], new_l[b], 0.0)
        summed = [front_f[b] + product_half(new_l[b], e_diag[b]) for b in span]
        for b in span:
            r_buf[row, b] = jnp.where(valid[b], product(inv_d[b], summed[b]), 0.0)

        for k in range(1, count_rows):
            to = lax.rem(row + count_rows - k, count_rows)
            remote(r_buf.at[row], r_buf.at[row], r_send.at[k], r_recv.at[row], to, col).start()
        send_own_l()

    loop(early, chunks, cross)

    lag = min(LAG, chunks - 1)

    def handled(src):
        before = ((level | behind) & (src == left_col)) | (behind & (src == lax.rem(col + count_cols - 2, count_cols)))
        return before | (src == col) | jnp.logical_not(is_active(row, src))

    def handle_at(src):
        p = phase_of(row, src)
        base = jnp.where(p == count_rows - 1, HANDLE_AT["ahead"], jnp.where(p == 0, HANDLE_AT["level"], HANDLE_AT["behind"]))
        return jnp.minimum(base + jnp.where(lax.rem(src + col, 2) == 0, 0, HANDLE_HOP), lag)

    def collect():
        for offset in range(1, -2, -1):
            src = lax.rem(col + offset + count_rows, count_rows)
            taken = ((level | behind) & (src == row_ahead)) | (behind & (src == row_level)) | (src == row)

            @pl.when(jnp.logical_not(taken))
            def _():
                wait_r(src)

        for b in range(cols_dev):
            for k, offset in enumerate((1, 0, -1)):
                hi, lo = split(r_buf[lax.rem(col + offset + count_rows, count_rows), b])
                r_cat[b, k * TILE : (k + 1) * TILE, :TILE] = hi
                r_cat[b, k * TILE : (k + 1) * TILE, TILE:] = lo

        def gather(a):
            for k, offset in enumerate((1, 0, -1)):
                m = a * count_rows + row - offset
                at = jnp.clip(m, 0, blocks - 1)
                tile = l_buf[lax.rem(at, count_cols), at // count_cols]
                hi, lo = split(jnp.where((m >= 0) & (m < blocks), tile, 0.0))
                l_cat[a, :TILE, k * TILE : (k + 1) * TILE] = hi
                l_cat[a, TILE:, k * TILE : (k + 1) * TILE] = lo

        loop(0, rows_dev, gather)

        @pl.when(jnp.logical_not(behind))
        def _():
            for copy in big_loads[:4]:
                copy.wait()

        for copy in big_loads[4:]:
            copy.wait()

    right_side, left_side = lax.rem(col, 2), 1 - lax.rem(col, 2)
    up_side, down_side = 1 - lax.rem(row, 2), lax.rem(row, 2)
    first_relay = jnp.where(col == count_cols - 1, offsets[1] if cols_dev > 1 else chunks, 0)

    def right_chunk(b, q):
        slot = jnp.minimum(b + at_last, cols_dev - 1)
        return chunk_of(slot, q)

    def left_chunk(b, q):
        slot = jnp.maximum(b - (col == 0).astype(jnp.int32), 0)
        return chunk_of(slot, q)

    def need(m):
        b, q = where_is(m)
        at = jnp.where(even_col, left_chunk(b, q), right_chunk(b, q))
        return jnp.where((col == count_cols - 1) & (b == cols_dev - 1), chunks - 1, at)

    def be_tile(side, which, b, a, height):
        at = jnp.clip(a, 0, height - 1)
        return be_buf[side, pick(b, offsets) + at // unit, which, lax.rem(at, unit)]

    def update(m):
        b, q = where_is(m)
        height = pick(b, tall)
        whole_be(0, m).wait_recv()
        lo = jnp.where(m == 0, 0, jnp.minimum(m + 1, chunks))
        loop(lo, jnp.minimum(m + 2, chunks), lambda n: whole_be(1, n).wait_recv())
        lo = jnp.where(m == 0, first_relay, need(jnp.maximum(m - 1, 0)) + 1)
        loop(lo, need(m) + 1, lambda n: whole_ad(1, n).wait_recv())
        at_right, at_left = right_chunk(b, q), left_chunk(b, q)
        j = b * count_cols + col
        for t in range(unit):
            a = q * unit + t
            i = a * count_rows + row
            up_a, down_a = a - (row == 0).astype(jnp.int32), a + (row == count_rows - 1).astype(jnp.int32)

            def apply(near_edge):
                def masked(tile, keep):
                    return jnp.where(keep, tile, jnp.zeros_like(tile)) if near_edge else tile

                def wide(which, own):
                    return jnp.concatenate(
                        [
                            ad_buf[right_side, at_right, which, t],
                            masked(own[a, b], i < j),
                            masked(ad_buf[left_side, at_left, which, t], i < j - 1),
                        ],
                        axis=1,
                    )

                def high(which, own):
                    return jnp.concatenate(
                        [
                            be_tile(up_side, which, b, up_a, height),
                            masked(own[a, b], i < j),
                            masked(be_tile(down_side, which, b, down_a, height), i < j - 1),
                        ],
                        axis=0,
                    )

                first = dot(jnp.concatenate([wide(0, a_ref), wide(1, d_ref)], axis=0), r_cat[b])
                second = dot(l_cat[a], jnp.concatenate([high(0, b_ref), high(1, e_ref)], axis=1))
                c_ref[a, b] = c_ref[a, b] - (first[:TILE, :TILE] + first[:TILE, TILE:]) + (second[:TILE, :TILE] + second[TILE:, :TILE])
                f_ref[a, b] = f_ref[a, b] - (first[TILE:, :TILE] + first[TILE:, TILE:]) + (second[:TILE, TILE:] + second[TILE:, TILE:])

            pl.when(i < j - 1)(lambda: apply(False))
            pl.when((i == j) | (i == j - 1))(lambda: apply(True))

    def done_by(n):
        return jnp.clip((n - lag + 1) * 3, 0, jnp.maximum(n - 1, 0))

    def wrapped_by(n):
        return jnp.where(wraps, jnp.clip((n - min(WRAP_LAG, chunks - 1) + 1) * 2, 0, jnp.maximum(n + 1, 0)), 0)

    def main(n):
        loop(jnp.maximum(early, jnp.where(n == 0, 0, n + IN_FLIGHT)), jnp.minimum(n + IN_FLIGHT + 1, chunks), swap)
        pl.when((n >= sent) & jnp.logical_not(wraps))(lambda: relay(n))
        loop(wrapped_by(n - 1), wrapped_by(n), relay)
        loop(0, count_cols, lambda src: pl.when((n == handle_at(src)) & jnp.logical_not(handled(src)))(lambda: handle(src)))
        pl.when(n == lag)(collect)
        loop(done_by(n - 1), done_by(n), update)

    loop(0, chunks, main)
    loop(wrapped_by(chunks - 1), jnp.where(wraps, chunks, 0), relay)
    loop(done_by(chunks - 1), chunks, update)

    copies = [local(r_buf.at[row], r_out, load_sem.at[14]), local(l_buf.at[col], l_out, load_sem.at[15])]
    for copy in copies:
        copy.start()

    def drain(n):
        whole_ad(0, n).wait_send()
        pl.when(relay_sent(n))(lambda: whole_ad(1, n).wait_send())
        whole_be(0, n).wait_send()
        whole_be(1, n).wait_send()

    loop(0, chunks, drain)

    def wait_sent(ref, sem):
        remote(ref, ref, sem, r_recv.at[0], row, col).wait_send()

    def wait_tiles_sent(ref, sem, short):
        pl.when(jnp.logical_not(short))(lambda: wait_sent(ref, sem))
        if cols_dev > 1:
            pl.when(short)(lambda: wait_sent(ref.at[pl.ds(0, cols_dev - 1)], sem))

    @pl.when(level)
    def _():
        wait_tiles_sent(a_diag, small_send.at[0], col == 0)
        wait_tiles_sent(a_diag, small_send.at[1], col == count_cols - 1)
        wait_sent(e_diag, small_send.at[2])
        wait_sent(e_diag, small_send.at[3])

    @pl.when(feeder)
    def _():
        wait_tiles_sent(ad_right, small_send.at[4], col == 0)
        wait_sent(be_up, small_send.at[5])

    @pl.when(active)
    def _():
        for k in range(1, count_rows):
            wait_sent(r_buf.at[row], r_send.at[k])

        for k, (when, _) in enumerate(own_routes()):
            maybe(when, lambda: wait_sent(l_buf.at[col], l_own_send.at[k]))

    def drain_l(src):
        pl.when(is_active(row, src) & ((src == col) | across(src)))(lambda: wait_sent(l_buf.at[src], l_send.at[src]))

    loop(0, count_cols, drain_l)

    for copy in copies:
        copy.wait()


def place_kernel(count_rows, count_cols, r_ref, l_ref, r_out, l_out):
    cols_dev = r_out.shape[1]
    row, col = lax.axis_index("row"), lax.axis_index("col")
    phase = lax.rem(col - row + count_rows, count_rows)
    active = (phase == count_rows - 1) | (phase <= 1)
    front = jnp.where(phase == count_rows - 1, 1, -phase)
    for b in range(cols_dev):
        here = active & (pl.program_id(0) * count_rows + row == b * count_cols + col + front)
        r_out[0, b] = jnp.where(here, r_ref[b], 0.0)
        l_out[0, b] = jnp.where(here, l_ref[b], 0.0)


def body(*args):
    count_rows = lax.axis_size("row")
    count_cols = lax.axis_size("col")
    row, col = lax.axis_index("row"), lax.axis_index("col")
    wide = [x.transpose(0, 2, 1, 3) for x in args[:6]]
    rows_dev, cols_dev = wide[0].shape[:2]
    blocks = rows_dev * count_rows
    tall = heights(rows_dev, cols_dev, count_rows, count_cols)
    unit = math.gcd(*tall)
    chunks = sum(tall) // unit
    anywhere, inside = pl.BlockSpec(memory_space=pl.ANY), pl.BlockSpec(memory_space=pltpu.VMEM)
    whole, few = (rows_dev, cols_dev, TILE, TILE), (cols_dev, TILE, TILE)
    f32, bf16 = jnp.float32, jnp.bfloat16
    dma = pltpu.SemaphoreType.DMA
    new_c, new_f, new_r, new_l = pl.pallas_call(
        functools.partial(kernel, count_rows, count_cols, unit, tall),
        in_specs=[anywhere] * 9 + [inside] + [anywhere] * 3 + [inside],
        out_specs=[inside, inside, anywhere, anywhere],
        out_shape=[pltpu.VMEM(whole, f32)] * 2 + [jax.ShapeDtypeStruct(few, f32)] * 2,
        scratch_shapes=[pltpu.VMEM(whole, bf16)] * 4
        + [pltpu.VMEM((2, chunks, 2, unit, TILE, TILE), bf16)] * 2
        + [
            pltpu.VMEM((count_rows,) + few, f32),
            pltpu.VMEM((count_cols,) + few, f32),
            pltpu.VMEM((cols_dev, 3 * TILE, 2 * TILE), bf16),
            pltpu.VMEM((rows_dev, 2 * TILE, 3 * TILE), bf16),
        ]
        + [pltpu.VMEM(few, f32)] * 8
        + [pltpu.VMEM(few, bf16)] * 2
        + [pltpu.VMEM((cols_dev, 2, TILE, TILE), bf16)] * 2
        + [dma((2, chunks))] * 4
        + [dma((count_rows,)), dma((count_rows,)), dma((count_cols,)), dma((count_cols,)), dma((count_cols,)), dma((6,)), dma((4,)), dma((16,))],
        compiler_params=pltpu.CompilerParams(collective_id=0, has_side_effects=True, vmem_limit_bytes=48 * 1024 * 1024),
        name="fronts",
    )(*wide, *args[6:])

    out_r, out_l = pl.pallas_call(
        functools.partial(place_kernel, count_rows, count_cols),
        grid=(rows_dev,),
        in_specs=[inside] * 2,
        out_specs=[pl.BlockSpec((1, cols_dev, TILE, TILE), lambda k: (k, 0, 0, 0))] * 2,
        out_shape=[jax.ShapeDtypeStruct(whole, f32)] * 2,
        cost_estimate=pl.CostEstimate(flops=4 * 10**7, bytes_accessed=8 * math.prod(whole), transcendentals=0),
        name="place",
    )(new_r, new_l)
    return tuple(x.transpose(0, 2, 1, 3) for x in (new_c, new_f, out_r, out_l))


def solution(mesh):
    grid = P(None, "row", None, "col")
    left, right = P(None, "row", None), P(None, "col", None)
    in_specs = (grid,) * 6 + (left,) * 3 + (P(None, "row"),) + (right,) * 3 + (P(None, "col"),)
    return jax.shard_map(body, mesh=mesh, in_specs=in_specs, out_specs=(grid,) * 4, check_vma=False)
```

```python
import functools
import math

import jax
import jax.numpy as jnp
from jax import lax
from jax.experimental import pallas as pl
from jax.experimental.pallas import tpu as pltpu
from jax.sharding import PartitionSpec as P

TILE = 128
MESH = pl.DeviceIdType.MESH
EARLY_SENDS = {"ahead": 2, "level": 7, "behind": 12}
EARLY_RELAYS = {"ahead": 0, "level": 1, "behind": 4}
LAG = 15
WRAP_LAG = 9
HANDLE_AT = {"ahead": 5, "level": 8, "behind": 12}
HANDLE_HOP = 3
IN_FLIGHT = 5


def heights(rows_dev, cols_dev, count_rows, count_cols):
    return [min(rows_dev, (b * count_cols + count_cols - 1) // count_rows + 1) for b in range(cols_dev)]


def split(value):
    hi = value.astype(jnp.bfloat16)
    return hi, (value - hi.astype(jnp.float32)).astype(jnp.bfloat16)


def dot(left, right):
    return jnp.dot(left, right, preferred_element_type=jnp.float32)


def product(left, right):
    left_hi, left_lo = split(left)
    right_hi, right_lo = split(right)
    return dot(
        jnp.concatenate([left_hi, left_lo, left_hi], axis=1), jnp.concatenate([right_hi, right_hi, right_lo], axis=0)
    )


def half_product(exact, value):
    return dot(jnp.concatenate([exact, exact], axis=1), jnp.concatenate(split(value), axis=0))


def product_half(value, exact):
    return dot(jnp.concatenate(split(value), axis=1), jnp.concatenate([exact, exact], axis=0))


def kernel(
    count_rows, count_cols, unit, tall,
    c_in, f_in, a_in, d_in, b_in, e_in, dinv_in, vec_left_in, back_left_in, eig_left_ref, inv_e_in, vec_right_in, back_right_in, eig_right_ref,
    c_ref, f_ref, r_out, l_out,
    a_ref, d_ref, b_ref, e_ref, ad_buf, be_buf, r_buf, l_buf, r_cat, l_cat,
    front_c, front_f, inv_d, vec_left, back_left, inv_e, vec_right, back_right, a_diag, e_diag, ad_right, be_up,
    ad_send, ad_recv, be_send, be_recv, r_send, r_recv, l_send, l_own_send, l_recv, small_send, small_recv, load_sem,
):
    rows_dev, cols_dev = c_ref.shape[:2]
    blocks = rows_dev * count_rows
    row, col = lax.axis_index("row"), lax.axis_index("col")
    pieces = [n // unit for n in tall]
    offsets = [sum(pieces[:b]) for b in range(cols_dev)]
    chunks = sum(pieces)

    def where_is(n):
        b = sum((n >= offset).astype(jnp.int32) for offset in offsets[1:]) if cols_dev > 1 else jnp.int32(0)
        return b, n - pick(b, offsets)

    def pick(b, values):
        out = jnp.int32(values[0])
        for k in range(1, len(values)):
            out = jnp.where(b == k, values[k], out)
        return out

    def chunk_of(b, q):
        return pick(b, offsets) + jnp.minimum(q, pick(b, pieces) - 1)

    phase = lax.rem(col - row + count_rows, count_rows)
    ahead, level, behind = phase == count_rows - 1, phase == 0, phase == 1
    active = ahead | level | behind
    feeder = (phase == 1) | (phase == 2)
    front = jnp.where(ahead, 1, -phase)
    mine, valid = [], []
    for b in range(cols_dev):
        i = b * count_cols + col + front
        valid.append(active & (i >= 0) & (i < blocks))
        mine.append(jnp.clip(i, 0, blocks - 1) // count_rows)

    partner_row = row + 1 - 2 * lax.rem(row, 2)
    cross_row = lax.rem(row + jnp.where(lax.rem(row, 2) == 0, count_rows - 1, 1), count_rows)
    partner_col = col + 1 - 2 * lax.rem(col, 2)
    relay_col = lax.rem(col + jnp.where(lax.rem(col, 2) == 0, 2, count_cols - 2), count_cols)
    even_col = lax.rem(col, 2) == 0
    left_col, right_col = lax.rem(col + count_cols - 1, count_cols), lax.rem(col + 1, count_cols)
    up_row, down_row = lax.rem(row + count_rows - 1, count_rows), lax.rem(row + 1, count_rows)

    def phase_of(r, c):
        return lax.rem(c - r + count_rows, count_rows)

    def is_active(r, c):
        p = phase_of(r, c)
        return (p == count_rows - 1) | (p == 0) | (p == 1)

    def remote(src, dst, send, recv, r, c):
        return pltpu.make_async_remote_copy(
            src_ref=src, dst_ref=dst, send_sem=send, recv_sem=recv, device_id=(r, c), device_id_type=MESH
        )

    def local(src, dst, sem):
        return pltpu.make_async_copy(src, dst, sem)

    solve_loads = []
    for b in range(cols_dev):
        for k, (src, dst) in enumerate([(c_in, front_c), (f_in, front_f)]):
            solve_loads.append(local(src.at[mine[b], b], dst.at[b], load_sem.at[k]))
        for k, (src, dst) in enumerate([(dinv_in, inv_d), (vec_left_in, vec_left), (back_left_in, back_left)]):
            solve_loads.append(local(src.at[mine[b]], dst.at[b], load_sem.at[2 + k]))
    fixed_loads = [
        local(src, dst, load_sem.at[5 + k])
        for k, (src, dst) in enumerate([(inv_e_in, inv_e), (vec_right_in, vec_right), (back_right_in, back_right)])
    ]
    for copy in solve_loads + fixed_loads:
        copy.start()

    barrier = pltpu.get_barrier_semaphore()
    for k in range(1, count_rows):
        pl.semaphore_signal(barrier, inc=1, device_id=(lax.rem(row + k, count_rows), col), device_id_type=MESH)
    for k in range(1, count_cols):
        pl.semaphore_signal(barrier, inc=1, device_id=(row, lax.rem(col + k, count_cols)), device_id_type=MESH)
    pl.semaphore_wait(barrier, count_rows + count_cols - 2)

    @pl.when(level)
    def _():
        for b in range(cols_dev):
            local(a_in.at[mine[b], b], a_diag.at[b], small_recv.at[0]).start()
            local(e_in.at[mine[b], b], e_diag.at[b], small_recv.at[1]).start()
        for b in range(cols_dev):
            at = b - (col == 0).astype(jnp.int32)

            @pl.when(at >= 0)
            def _():
                remote(a_in.at[mine[b], b], a_diag.at[jnp.maximum(at, 0)], small_send.at[0], small_recv.at[0], row, left_col).start()

            to = b + (col == count_cols - 1).astype(jnp.int32)

            @pl.when(to < cols_dev)
            def _():
                remote(a_in.at[mine[b], b], a_diag.at[jnp.minimum(to, cols_dev - 1)], small_send.at[1], small_recv.at[0], row, right_col).start()

            remote(e_in.at[mine[b], b], e_diag.at[b], small_send.at[2], small_recv.at[1], down_row, col).start()
            remote(e_in.at[mine[b], b], e_diag.at[b], small_send.at[3], small_recv.at[1], up_row, col).start()

    @pl.when(feeder)
    def _():
        for b in range(cols_dev):
            at = b - (col == 0).astype(jnp.int32)

            @pl.when(at >= 0)
            def _():
                for k, src in enumerate((a_in, d_in)):
                    remote(src.at[mine[b], b], ad_right.at[jnp.maximum(at, 0), k], small_send.at[4], small_recv.at[2], row, left_col).start()

            for k, src in enumerate((b_in, e_in)):
                remote(src.at[mine[b], b], be_up.at[b, k], small_send.at[5], small_recv.at[3], down_row, col).start()

    def swap(n):
        b, q = where_is(n)
        for k, src in enumerate((a_in, d_in)):
            remote(src.at[pl.ds(q * unit, unit), b], ad_buf.at[0, n, k], ad_send.at[0, n], ad_recv.at[0, n], row, partner_col).start()

    def cross(n):
        b, q = where_is(n)
        for k, src in enumerate((b_in, e_in)):
            remote(src.at[pl.ds(q * unit, unit), b], be_buf.at[1, n, k], be_send.at[1, n], be_recv.at[1, n], cross_row, col).start()

    def near(n):
        b, q = where_is(n)
        for k, src in enumerate((b_in, e_in)):
            remote(src.at[pl.ds(q * unit, unit), b], be_buf.at[0, n, k], be_send.at[0, n], be_recv.at[0, n], partner_row, col).start()

    def whole_ad(side, n):
        return remote(ad_buf.at[side, n], ad_buf.at[side, n], ad_send.at[side, n], ad_recv.at[side, n], row, partner_col)

    def whole_be(side, n):
        return remote(be_buf.at[side, n], be_buf.at[side, n], be_send.at[side, n], be_recv.at[side, n], partner_row, col)

    def relay_sent(n):
        b, _ = where_is(n)
        skip = ((col == count_cols - 2) & (b == cols_dev - 1)) | ((col == 1) & (b == 0))
        return jnp.logical_not(skip)

    def relay(n):
        whole_ad(0, n).wait_recv()

        @pl.when(relay_sent(n))
        def _():
            remote(ad_buf.at[0, n], ad_buf.at[1, n], ad_send.at[1, n], ad_recv.at[1, n], row, relay_col).start()

    def loop(lo, hi, body):
        lax.fori_loop(lo, hi, lambda n, _: (body(n), 0)[1], 0)

    early = jnp.int32(min(IN_FLIGHT, chunks))
    sent = jnp.int32(0)
    for name, flag in (("ahead", ahead), ("level", level), ("behind", behind)):
        early = jnp.where(flag, min(EARLY_SENDS[name], chunks), early)
        sent = jnp.where(flag, min(EARLY_RELAYS[name], chunks), sent)

    wraps = (col == 1) | (col == count_cols - 2)
    sent = jnp.where(wraps, 0, sent)
    loop(0, early, swap)
    loop(0, early, cross)
    loop(0, chunks, near)
    big_loads = [
        local(src, dst, load_sem.at[8 + k])
        for k, (src, dst) in enumerate([(a_in, a_ref), (d_in, d_ref), (b_in, b_ref), (e_in, e_ref), (c_in, c_ref), (f_in, f_ref)])
    ]
    for copy in big_loads:
        copy.start()
    loop(0, sent, relay)

    for k, dst in enumerate((front_c, front_f, inv_d, vec_left, back_left)):
        local(dst, dst, load_sem.at[k]).wait()
    for copy in fixed_loads:
        copy.wait()

    at_last = (col == count_cols - 1).astype(jnp.int32)

    def wait_tiles(ref, sem, short):
        @pl.when(jnp.logical_not(short))
        def _():
            local(ref, ref, sem).wait()

        if cols_dev > 1:

            @pl.when(short)
            def _():
                part = ref.at[pl.ds(0, cols_dev - 1)]
                local(part, part, sem).wait()

    @pl.when(active)
    def _():
        short = (ahead & (col == count_cols - 1)) | (behind & (col == 0))
        wait_tiles(a_diag, small_recv.at[0], short)
        local(e_diag, e_diag, small_recv.at[1]).wait()

    def got_l(c, b):
        back = (c < 0).astype(jnp.int32)
        slot = b - back
        tile = l_buf[lax.rem(c + count_cols, count_cols), jnp.maximum(slot, 0)]
        return jnp.where(slot >= 0, tile, 0.0)

    def wait_r(r):
        remote(r_buf.at[r], r_buf.at[r], r_send.at[0], r_recv.at[r], row, col).wait_recv()

    def wait_l(c):
        remote(l_buf.at[c], l_buf.at[c], l_send.at[0], l_recv.at[c], row, col).wait_recv()

    def direct(src, dst):
        p = phase_of(row, src)
        return (lax.rem(src, 2) == 1) & (dst == lax.rem(src + 1, count_cols)) & ((p == count_rows - 1) | (p == 0))

    def own_routes():
        order = [k for n in range(1, count_cols // 4 + 1) for k in dict.fromkeys((n, count_cols // 2 - n))]
        routes = [(direct(col, right_col), right_col)] + [(None, lax.rem(col + 2 * k, count_cols)) for k in order]
        return routes

    def across(src):
        return (src != col) & (lax.rem(src + col, 2) == 0) & jnp.logical_not(direct(src, partner_col))

    def maybe(when, run):
        return run() if when is None else pl.when(when)(run)

    def send_l(src):
        remote(l_buf.at[src], l_buf.at[src], l_send.at[src], l_recv.at[src], row, partner_col).start()

    def send_own_l():
        send_l(col)
        for k, (when, to) in enumerate(own_routes()):
            maybe(when, lambda: remote(l_buf.at[col], l_buf.at[col], l_own_send.at[k], l_recv.at[col], row, to).start())

    def handle(src):
        wait_l(src)
        pl.when(across(src))(lambda: send_l(src))

    def absorb(ad, be, right, left):
        for b in range(cols_dev):
            a_tile, d_tile = ad(b)
            b_tile, e_tile = be(b)
            value_r, value_l = right(b), left(b)
            front_c[b] = front_c[b] - half_product(a_tile, value_r) + product_half(value_l, b_tile)
            front_f[b] = front_f[b] - half_product(d_tile, value_r) + product_half(value_l, e_tile)

    row_ahead, row_level = lax.rem(col + 1, count_rows), lax.rem(col, count_rows)
    col_first = jnp.where(level, col - 1, col - 2)

    @pl.when(level | behind)
    def _():
        wait_tiles(ad_right, small_recv.at[2], col == count_cols - 1)
        local(be_up, be_up, small_recv.at[3]).wait()
        wait_r(row_ahead)
        handle(lax.rem(col_first + count_cols, count_cols))

        def right_tiles(b):
            tiles = ad_right[b, 0], ad_right[b, 1]
            if b < cols_dev - 1:
                return tiles
            return tuple(jnp.where(col == count_cols - 1, jnp.zeros_like(tile), tile) for tile in tiles)

        absorb(right_tiles, lambda b: (be_up[b, 0], be_up[b, 1]), lambda b: r_buf[row_ahead, b], lambda b: got_l(col_first, b))

    @pl.when(behind)
    def _():
        for copy in big_loads[:4]:
            copy.wait()
        wait_r(row_level)
        handle(left_col)
        absorb(
            lambda b: (a_ref[mine[b], b], d_ref[mine[b], b]),
            lambda b: (b_ref[mine[b], b], e_ref[mine[b], b]),
            lambda b: r_buf[row_level, b],
            lambda b: got_l(col - 1, b),
        )

    @pl.when(active)
    def _():
        span = range(cols_dev)
        coupled = [half_product(a_diag[b], inv_d[b]) for b in span]
        merged = [front_c[b] - product(coupled[b], front_f[b]) for b in span]
        merged = [product(merged[b], inv_e[b]) for b in span]
        spectral = [product(back_left[b], merged[b]) for b in span]
        spectral = [product(spectral[b], vec_right[b]) for b in span]
        for b in span:
            eig = jnp.broadcast_to(eig_left_ref[pl.ds(mine[b], 1), :], (TILE, TILE)).T
            spectral[b] = spectral[b] / (eig - eig_right_ref[pl.ds(b, 1), :])
        new_l = [product(vec_left[b], spectral[b]) for b in span]
        new_l = [product(new_l[b], back_right[b]) for b in span]
        for b in span:
            l_buf[col, b] = jnp.where(valid[b], new_l[b], 0.0)
        summed = [front_f[b] + product_half(new_l[b], e_diag[b]) for b in span]
        for b in span:
            r_buf[row, b] = jnp.where(valid[b], product(inv_d[b], summed[b]), 0.0)

        for k in range(1, count_rows):
            to = lax.rem(row + count_rows - k, count_rows)
            remote(r_buf.at[row], r_buf.at[row], r_send.at[k], r_recv.at[row], to, col).start()
        send_own_l()

    loop(early, chunks, cross)

    lag = min(LAG, chunks - 1)

    def handled(src):
        before = ((level | behind) & (src == left_col)) | (behind & (src == lax.rem(col + count_cols - 2, count_cols)))
        return before | (src == col) | jnp.logical_not(is_active(row, src))

    def handle_at(src):
        p = phase_of(row, src)
        base = jnp.where(p == count_rows - 1, HANDLE_AT["ahead"], jnp.where(p == 0, HANDLE_AT["level"], HANDLE_AT["behind"]))
        return jnp.minimum(base + jnp.where(lax.rem(src + col, 2) == 0, 0, HANDLE_HOP), lag)

    def collect():
        for offset in range(1, -2, -1):
            src = lax.rem(col + offset + count_rows, count_rows)
            taken = ((level | behind) & (src == row_ahead)) | (behind & (src == row_level)) | (src == row)

            @pl.when(jnp.logical_not(taken))
            def _():
                wait_r(src)

        for b in range(cols_dev):
            for k, offset in enumerate((1, 0, -1)):
                hi, lo = split(r_buf[lax.rem(col + offset + count_rows, count_rows), b])
                r_cat[b, k * TILE : (k + 1) * TILE, :TILE] = hi
                r_cat[b, k * TILE : (k + 1) * TILE, TILE:] = lo

        def gather(a):
            for k, offset in enumerate((1, 0, -1)):
                m = a * count_rows + row - offset
                at = jnp.clip(m, 0, blocks - 1)
                tile = l_buf[lax.rem(at, count_cols), at // count_cols]
                hi, lo = split(jnp.where((m >= 0) & (m < blocks), tile, 0.0))
                l_cat[a, :TILE, k * TILE : (k + 1) * TILE] = hi
                l_cat[a, TILE:, k * TILE : (k + 1) * TILE] = lo

        loop(0, rows_dev, gather)

        @pl.when(jnp.logical_not(behind))
        def _():
            for copy in big_loads[:4]:
                copy.wait()

        for copy in big_loads[4:]:
            copy.wait()

    right_side, left_side = lax.rem(col, 2), 1 - lax.rem(col, 2)
    up_side, down_side = 1 - lax.rem(row, 2), lax.rem(row, 2)
    first_relay = jnp.where(col == count_cols - 1, offsets[1] if cols_dev > 1 else chunks, 0)

    def right_chunk(b, q):
        slot = jnp.minimum(b + at_last, cols_dev - 1)
        return chunk_of(slot, q)

    def left_chunk(b, q):
        slot = jnp.maximum(b - (col == 0).astype(jnp.int32), 0)
        return chunk_of(slot, q)

    def need(m):
        b, q = where_is(m)
        at = jnp.where(even_col, left_chunk(b, q), right_chunk(b, q))
        return jnp.where((col == count_cols - 1) & (b == cols_dev - 1), chunks - 1, at)

    def be_tile(side, which, b, a, height):
        at = jnp.clip(a, 0, height - 1)
        return be_buf[side, pick(b, offsets) + at // unit, which, lax.rem(at, unit)]

    def update(m):
        b, q = where_is(m)
        height = pick(b, tall)
        whole_be(0, m).wait_recv()
        lo = jnp.where(m == 0, 0, jnp.minimum(m + 1, chunks))
        loop(lo, jnp.minimum(m + 2, chunks), lambda n: whole_be(1, n).wait_recv())
        lo = jnp.where(m == 0, first_relay, need(jnp.maximum(m - 1, 0)) + 1)
        loop(lo, need(m) + 1, lambda n: whole_ad(1, n).wait_recv())
        at_right, at_left = right_chunk(b, q), left_chunk(b, q)
        j = b * count_cols + col
        for t in range(unit):
            a = q * unit + t
            i = a * count_rows + row
            up_a, down_a = a - (row == 0).astype(jnp.int32), a + (row == count_rows - 1).astype(jnp.int32)

            def apply(near_edge):
                def masked(tile, keep):
                    return jnp.where(keep, tile, jnp.zeros_like(tile)) if near_edge else tile

                def wide(which, own):
                    return jnp.concatenate(
                        [
                            ad_buf[right_side, at_right, which, t],
                            masked(own[a, b], i < j),
                            masked(ad_buf[left_side, at_left, which, t], i < j - 1),
                        ],
                        axis=1,
                    )

                def high(which, own):
                    return jnp.concatenate(
                        [
                            be_tile(up_side, which, b, up_a, height),
                            masked(own[a, b], i < j),
                            masked(be_tile(down_side, which, b, down_a, height), i < j - 1),
                        ],
                        axis=0,
                    )

                first = dot(jnp.concatenate([wide(0, a_ref), wide(1, d_ref)], axis=0), r_cat[b])
                second = dot(l_cat[a], jnp.concatenate([high(0, b_ref), high(1, e_ref)], axis=1))
                c_ref[a, b] = c_ref[a, b] - (first[:TILE, :TILE] + first[:TILE, TILE:]) + (second[:TILE, :TILE] + second[TILE:, :TILE])
                f_ref[a, b] = f_ref[a, b] - (first[TILE:, :TILE] + first[TILE:, TILE:]) + (second[:TILE, TILE:] + second[TILE:, TILE:])

            pl.when(i < j - 1)(lambda: apply(False))
            pl.when((i == j) | (i == j - 1))(lambda: apply(True))

    def done_by(n):
        return jnp.clip((n - lag + 1) * 3, 0, jnp.maximum(n - 1, 0))

    def wrapped_by(n):
        return jnp.where(wraps, jnp.clip((n - min(WRAP_LAG, chunks - 1) + 1) * 2, 0, jnp.maximum(n + 1, 0)), 0)

    def main(n):
        loop(jnp.maximum(early, jnp.where(n == 0, 0, n + IN_FLIGHT)), jnp.minimum(n + IN_FLIGHT + 1, chunks), swap)
        pl.when((n >= sent) & jnp.logical_not(wraps))(lambda: relay(n))
        loop(wrapped_by(n - 1), wrapped_by(n), relay)
        loop(0, count_cols, lambda src: pl.when((n == handle_at(src)) & jnp.logical_not(handled(src)))(lambda: handle(src)))
        pl.when(n == lag)(collect)
        loop(done_by(n - 1), done_by(n), update)

    loop(0, chunks, main)
    loop(wrapped_by(chunks - 1), jnp.where(wraps, chunks, 0), relay)
    loop(done_by(chunks - 1), chunks, update)

    copies = [local(r_buf.at[row], r_out, load_sem.at[14]), local(l_buf.at[col], l_out, load_sem.at[15])]
    for copy in copies:
        copy.start()

    def drain(n):
        whole_ad(0, n).wait_send()
        pl.when(relay_sent(n))(lambda: whole_ad(1, n).wait_send())
        whole_be(0, n).wait_send()
        whole_be(1, n).wait_send()

    loop(0, chunks, drain)

    def wait_sent(ref, sem):
        remote(ref, ref, sem, r_recv.at[0], row, col).wait_send()

    def wait_tiles_sent(ref, sem, short):
        pl.when(jnp.logical_not(short))(lambda: wait_sent(ref, sem))
        if cols_dev > 1:
            pl.when(short)(lambda: wait_sent(ref.at[pl.ds(0, cols_dev - 1)], sem))

    @pl.when(level)
    def _():
        wait_tiles_sent(a_diag, small_send.at[0], col == 0)
        wait_tiles_sent(a_diag, small_send.at[1], col == count_cols - 1)
        wait_sent(e_diag, small_send.at[2])
        wait_sent(e_diag, small_send.at[3])

    @pl.when(feeder)
    def _():
        wait_tiles_sent(ad_right, small_send.at[4], col == 0)
        wait_sent(be_up, small_send.at[5])

    @pl.when(active)
    def _():
        for k in range(1, count_rows):
            wait_sent(r_buf.at[row], r_send.at[k])

        for k, (when, _) in enumerate(own_routes()):
            maybe(when, lambda: wait_sent(l_buf.at[col], l_own_send.at[k]))

    def drain_l(src):
        pl.when(is_active(row, src) & ((src == col) | across(src)))(lambda: wait_sent(l_buf.at[src], l_send.at[src]))

    loop(0, count_cols, drain_l)

    for copy in copies:
        copy.wait()


def place_kernel(count_rows, count_cols, r_ref, l_ref, r_out, l_out):
    cols_dev = r_out.shape[1]
    row, col = lax.axis_index("row"), lax.axis_index("col")
    phase = lax.rem(col - row + count_rows, count_rows)
    active = (phase == count_rows - 1) | (phase <= 1)
    front = jnp.where(phase == count_rows - 1, 1, -phase)
    for b in range(cols_dev):
        here = active & (pl.program_id(0) * count_rows + row == b * count_cols + col + front)
        r_out[0, b] = jnp.where(here, r_ref[b], 0.0)
        l_out[0, b] = jnp.where(here, l_ref[b], 0.0)


def body(*args):
    count_rows = lax.axis_size("row")
    count_cols = lax.axis_size("col")
    row, col = lax.axis_index("row"), lax.axis_index("col")
    wide = [x.transpose(0, 2, 1, 3) for x in args[:6]]
    rows_dev, cols_dev = wide[0].shape[:2]
    blocks = rows_dev * count_rows
    tall = heights(rows_dev, cols_dev, count_rows, count_cols)
    unit = math.gcd(*tall)
    chunks = sum(tall) // unit
    anywhere, inside = pl.BlockSpec(memory_space=pl.ANY), pl.BlockSpec(memory_space=pltpu.VMEM)
    whole, few = (rows_dev, cols_dev, TILE, TILE), (cols_dev, TILE, TILE)
    f32, bf16 = jnp.float32, jnp.bfloat16
    dma = pltpu.SemaphoreType.DMA
    new_c, new_f, new_r, new_l = pl.pallas_call(
        functools.partial(kernel, count_rows, count_cols, unit, tall),
        in_specs=[anywhere] * 9 + [inside] + [anywhere] * 3 + [inside],
        out_specs=[inside, inside, anywhere, anywhere],
        out_shape=[pltpu.VMEM(whole, f32)] * 2 + [jax.ShapeDtypeStruct(few, f32)] * 2,
        scratch_shapes=[pltpu.VMEM(whole, bf16)] * 4
        + [pltpu.VMEM((2, chunks, 2, unit, TILE, TILE), bf16)] * 2
        + [
            pltpu.VMEM((count_rows,) + few, f32),
            pltpu.VMEM((count_cols,) + few, f32),
            pltpu.VMEM((cols_dev, 3 * TILE, 2 * TILE), bf16),
            pltpu.VMEM((rows_dev, 2 * TILE, 3 * TILE), bf16),
        ]
        + [pltpu.VMEM(few, f32)] * 8
        + [pltpu.VMEM(few, bf16)] * 2
        + [pltpu.VMEM((cols_dev, 2, TILE, TILE), bf16)] * 2
        + [dma((2, chunks))] * 4
        + [dma((count_rows,)), dma((count_rows,)), dma((count_cols,)), dma((count_cols,)), dma((count_cols,)), dma((6,)), dma((4,)), dma((16,))],
        compiler_params=pltpu.CompilerParams(collective_id=0, has_side_effects=True, vmem_limit_bytes=48 * 1024 * 1024),
        name="fronts",
    )(*wide, *args[6:])

    out_r, out_l = pl.pallas_call(
        functools.partial(place_kernel, count_rows, count_cols),
        grid=(rows_dev,),
        in_specs=[inside] * 2,
        out_specs=[pl.BlockSpec((1, cols_dev, TILE, TILE), lambda k: (k, 0, 0, 0))] * 2,
        out_shape=[jax.ShapeDtypeStruct(whole, f32)] * 2,
        cost_estimate=pl.CostEstimate(flops=4 * 10**7, bytes_accessed=8 * math.prod(whole), transcendentals=0),
        name="place",
    )(new_r, new_l)
    return tuple(x.transpose(0, 2, 1, 3) for x in (new_c, new_f, out_r, out_l))


def solution(mesh):
    grid = P(None, "row", None, "col")
    left, right = P(None, "row", None), P(None, "col", None)
    in_specs = (grid,) * 6 + (left,) * 3 + (P(None, "row"),) + (right,) * 3 + (P(None, "col"),)
    return jax.shard_map(body, mesh=mesh, in_specs=in_specs, out_specs=(grid,) * 4, check_vma=False)
```
